32 devices in a mesh: rep: 2 (over x), stretch: 2 (over core), tp: 8 (over z, y).
Axes of the slice: x: 2, y: 2, z: 4, core: 2. Of those that a mesh axis runs over, the one named last changes fastest.
Arguments:
- query: bfloat16 [4, 512, 3072], P(('rep', 'stretch'), 'tp'), parts along dimension 0, may hold values from -64 to 64
- stretch_kv: bfloat16 [2, 4, 512, 3072], P(None, ('rep', 'stretch'), 'tp'), parts along dimension 1, may hold values from -6 to 6
- history_kv: bfloat16 [2, 4096, 3072], P(None, ('rep', 'tp')), parts along dimension 1, may hold values from -6 to 6
- block_mask: int32 [4, 4, 8], P(('rep', 'stretch')), parts along dimension 0, may hold values from 0 to 1, as said below
- noise_level: int32 [4], P(('rep', 'stretch')), parts along dimension 0, may hold values from 0 to 999
- history_blocks: int32 [2], P('rep'), parts along dimension 0, may hold values from 1 to 16
- out_weight: bfloat16 [3072, 6144], P(None, 'tp'), may hold values from -0.109375 to 0.109375
- gate_table: float32 [1000, 6144], P(None, 'tp'), may hold values from -6 to 6
Outputs:
- mixed: bfloat16 [4, 512, 6144], P(('rep', 'stretch'), None, 'tp'), parts along dimension 0
The draws below stay inside these ranges and needn't reach their ends.
There are 2 independent parts, one for each index of `rep`. The reference program is written for one: setup_inputs(seed, part) draws one part's arguments, and reference() takes and returns one part's arrays. A program takes and returns all parts, laid end to end along the dimension named above; an argument that names none is the same for every part. Nothing has to cross between parts.
Inputs may be any that keep to these rules, and one draw needn't show every extreme that they name: block_mask[c, i, 4 + i] = 1 for every query block i; block_mask[0, i, j] = 0 for j < 4.
All inputs are finite; a program needn't handle non-finite values.
Results may differ from the reference program's by a relative error of at most 0.0049.
Values may be sent and summed in bfloat16 or wider, within the bound.
A program may use at most 128 MiB of HBM per device.

```python
import math
import jax
import jax.numpy as jnp
from jax import lax

D = 6144
H = 24
HD = 128
LEVELS = 1000
BLK = 128
CT = 512
QB = 4
HIST = 2048


def shared_draws(key):
    query_key = jax.random.fold_in(key, 101)
    history_key = jax.random.fold_in(key, 202)
    feature_width = H * HD
    history = jnp.clip(jax.random.normal(history_key, (2, HIST, feature_width), jnp.float32), -6.0, 6.0)
    queries = jnp.clip(2.0 * jax.random.normal(query_key, (2, CT, feature_width), jnp.float32), -12.0, 12.0)
    return (queries, history)


def draw_query(key, part):
    return shared_draws(key)[0].astype(jnp.bfloat16)


def draw_history_kv(key, part):
    return shared_draws(key)[1].astype(jnp.bfloat16)


def draw_block_mask(key, part):
    raw_bits = jax.random.randint(jax.random.fold_in(key, 404), (2, QB, 2 * QB), 0, 5)
    grid_rows = lax.broadcasted_iota(jnp.int32, (2, QB, 2 * QB), 1)
    grid_cols = lax.broadcasted_iota(jnp.int32, (2, QB, 2 * QB), 2)
    grid_stretches = lax.broadcasted_iota(jnp.int32, (2, QB, 2 * QB), 0)
    block_allow = jnp.where(raw_bits < 3, 1, 0)
    block_allow = jnp.where(grid_cols == grid_rows + QB, 1, block_allow)
    block_allow = jnp.where((grid_stretches == 0) & (grid_cols < QB), 0, block_allow)
    return block_allow.astype(jnp.int32)


def levels(rng, extent, shards, least, high):
    level = 1.0
    for position, parts in shards:
        heights = jax.random.uniform(jax.random.fold_in(jax.random.fold_in(rng, 6), position), (parts,), jnp.float32, least / len(shards), high / len(shards))
        level = level * jnp.repeat(jnp.exp(heights), extent[position] // parts).reshape((-1,) + (1,) * (len(extent) - 1 - position))
    return level


def bell_draw(own_key, dims, width, most, shards=(), kind=jnp.bfloat16):
    values = jax.random.normal(own_key, dims, jnp.float32) * width
    if len(shards) > 0:
        values = levels(own_key, dims, shards, -0.22, 0.18) * values
    return jnp.clip(values, min=-most, max=most).astype(kind)


def setup_inputs(seed: int = 0, part: int = 0) -> dict:
    key_list = jax.random.split(jax.random.key(seed), 9)
    own_keys = jax.random.split(jax.random.fold_in(key_list[8], part), 9)
    return {
        "query": draw_query(jax.random.fold_in(jax.random.fold_in(key_list[8], part), 71), part),
        "stretch_kv": bell_draw(own_keys[1], (2, 2, CT, H * HD), 1.0, 6.0, ((1, 2), (2, 8))),
        "history_kv": draw_history_kv(jax.random.fold_in(jax.random.fold_in(key_list[8], part), 71), part),
        "block_mask": draw_block_mask(jax.random.fold_in(jax.random.fold_in(key_list[8], part), 71), part),
        "noise_level": jax.random.randint(own_keys[4], (2,), 0, LEVELS).astype(jnp.int32),
        "history_blocks": jax.random.randint(own_keys[5], (1,), 1, HIST // BLK + 1).astype(jnp.int32),
        "out_weight": bell_draw(key_list[6], (H * HD, D), (H * HD) ** -0.5, 0.109375, ((1, 8),)),
        "gate_table": bell_draw(key_list[7], (LEVELS, D), 1.0, 6.0, ((1, 8),), jnp.float32),
    }


NEGATIVE = -1e+30

def single_head(triple_args, allowed):
    queries, key_rows, value_rows = triple_args
    scores = jnp.dot(queries, key_rows.T, preferred_element_type=jnp.float32) * (1.0 / math.sqrt(HD))
    scores = jnp.where(allowed, scores, NEGATIVE)
    row_peak = lax.optimization_barrier(jnp.max(scores, axis=1, keepdims=True))
    weights = jnp.where(allowed, jnp.exp(scores - row_peak), 0.0)
    weight_sum = lax.optimization_barrier(jnp.sum(weights, axis=1, keepdims=True))
    output = jnp.dot(weights, value_rows.astype(jnp.float32), precision=lax.Precision.HIGHEST) / weight_sum
    return output.astype(jnp.bfloat16)

def reference(query, stretch_kv, history_kv, block_mask, noise_level, history_blocks, out_weight, gate_table):
    history_live = jnp.arange(HIST, dtype=jnp.int32) < history_blocks[0] * BLK
    results = []
    for stretch_index in range(2):
        if stretch_index == 1:
            older_pair = stretch_kv[:, 0]
        else:
            older_pair = jnp.zeros_like(stretch_kv[:, 0])
        key_rows = jnp.concatenate([history_kv[0], older_pair[0], stretch_kv[0, stretch_index]], 0)
        value_rows = jnp.concatenate([history_kv[1], older_pair[1], stretch_kv[1, stretch_index]], 0)
        fresh = jnp.repeat(jnp.repeat(block_mask[stretch_index] > 0, BLK, axis=0), BLK, axis=1)
        allowed = jnp.concatenate([jnp.broadcast_to(history_live[None, :], (CT, HIST)), fresh], 1)
        key_count = key_rows.shape[0]
        head_queries = jnp.transpose(query[stretch_index].reshape(CT, H, HD), (1, 0, 2))
        head_keys = jnp.transpose(key_rows.reshape(key_count, H, HD), (1, 0, 2))
        head_values = jnp.transpose(value_rows.reshape(key_count, H, HD), (1, 0, 2))
        attended = lax.map(lambda triple_args: single_head(triple_args, allowed), (head_queries, head_keys, head_values))
        attended = jnp.transpose(attended, (1, 0, 2)).reshape(CT, H * HD)
        projected = jnp.dot(attended, out_weight, preferred_element_type=jnp.float32)
        gate_row = gate_table[noise_level[stretch_index]]
        results.append((projected * gate_row[None, :]).astype(jnp.bfloat16))
    return jnp.stack(results, 0)
```

```python
import functools
import math

import jax
import jax.numpy as jnp
from jax import lax
from jax.experimental import pallas as pl
from jax.experimental.pallas import tpu as pltpu
from jax.sharding import PartitionSpec as P

H = 24
HD = 128
BLK = 128


NEGATIVE = -1e30


def shifted(value, axis, steps):
    count = lax.axis_size(axis)
    first, last = (max(0, -steps), min(count, count - steps))
    return lax.ppermute(value, axis, [(source, source + steps) for source in range(first, last)])


def head_block(queries, key_rows, value_rows, allowed):
    key_count = key_rows.shape[0]
    head_count = queries.shape[1]
    key_heads = key_rows.reshape(key_count, head_count, HD)
    scores = jnp.einsum("qhd,khd->qhk", queries, key_heads, preferred_element_type=jnp.float32) * (
        1.0 / math.sqrt(HD)
    )
    scores = jnp.where(allowed[:, None, :], scores, NEGATIVE)
    row_peak = jnp.max(scores, axis=2)
    weights = jnp.where(allowed[:, None, :], jnp.exp(scores - row_peak[:, :, None]), 0.0)
    weight_sum = jnp.sum(weights, axis=2)
    output = None
    value_heads = value_rows.reshape(key_count, head_count, HD).astype(jnp.float32)
    output = jnp.einsum("qhk,khd->qhd", weights, value_heads, precision=lax.Precision.HIGHEST)
    return (row_peak, weight_sum, output)


def combine(earlier, later):
    row_peak = jnp.maximum(earlier[0], later[0])
    scale_one = jnp.exp(earlier[0] - row_peak)
    scale_two = jnp.exp(later[0] - row_peak)
    weight_sum = earlier[1] * scale_one + later[1] * scale_two
    output = None
    output = earlier[2] * scale_one[:, :, None] + later[2] * scale_two[:, :, None]
    return (row_peak, weight_sum, output)


def column_table(columns, block_count):
    return (columns[:, None] == jnp.arange(2 * block_count, dtype=jnp.int32)[None, :]).astype(
        jnp.float32
    )


def attend_all(
    queries,
    query_positions,
    fresh_keys,
    fresh_values,
    fresh_hot,
    mask_table,
    history_pair,
    history_live,
    span,
):
    row_count = queries.shape[0]
    head_count = queries.shape[1]
    block_count = mask_table.shape[0]
    query_hot = (
        (query_positions // BLK)[:, None] == jnp.arange(block_count, dtype=jnp.int32)[None, :]
    ).astype(jnp.float32)
    fresh_allowed = jnp.dot(jnp.dot(query_hot, mask_table), fresh_hot.T) > 0.5
    base_peak = jnp.full((row_count, head_count), NEGATIVE, jnp.float32)
    skipped = (
        base_peak,
        jnp.zeros((row_count, head_count), jnp.float32),
        jnp.zeros((row_count, head_count, HD), jnp.float32),
    )
    result = head_block(queries, fresh_keys, fresh_values, fresh_allowed)
    for sub_block in range(history_pair.shape[1] // span):
        lower_row = sub_block * span
        key_rows = history_pair[0, lower_row : lower_row + span]
        value_rows = history_pair[1, lower_row : lower_row + span]
        live_rows = history_live[lower_row : lower_row + span]
        allowed = jnp.broadcast_to(live_rows[None, :], (row_count, span))
        block_part = lax.cond(
            jnp.any(live_rows),
            lambda: head_block(queries, key_rows, value_rows, allowed),
            lambda: skipped,
        )
        result = combine(result, block_part)
    return result


def on_device(
    query, stretch_kv, history_kv, block_mask, noise_level, history_blocks, out_weight, gate_table
):
    tp_count = lax.axis_size("tp")
    tp_index = lax.axis_index("tp")
    local_rows = query.shape[1]
    feature_width = query.shape[2]
    history_rows = history_kv.shape[1]
    block_count = block_mask.shape[1]
    own_pair = stretch_kv[:, 0]
    older_pair = shifted(own_pair, "stretch", 1)
    mask_table = block_mask[0].astype(jnp.float32)
    live_limit = history_blocks[0] * BLK
    fresh_keys = jnp.concatenate([older_pair[0], own_pair[0]], 0)
    fresh_values = jnp.concatenate([older_pair[1], own_pair[1]], 0)
    own_positions = tp_index * local_rows + jnp.arange(local_rows, dtype=jnp.int32)
    fresh_hot = column_table(
        jnp.concatenate([own_positions // BLK, block_count + own_positions // BLK], 0), block_count
    )
    history_positions = tp_index * history_rows + jnp.arange(history_rows, dtype=jnp.int32)
    history_live = history_positions < live_limit
    piece = lax.all_gather(query[0], "tp", axis=0, tiled=True)
    row_count = piece.shape[0]
    positions = jnp.arange(row_count, dtype=jnp.int32)
    row_peak, weight_sum, output = attend_all(
        piece.reshape(row_count, H, HD),
        positions,
        fresh_keys,
        fresh_values,
        fresh_hot,
        mask_table,
        history_kv,
        history_live,
        BLK,
    )
    got_outputs, got_peaks, got_sums = (
        lax.all_to_all(
            output.reshape(tp_count, local_rows, H, HD),
            "tp",
            split_axis=0,
            concat_axis=0,
            tiled=True,
        ),
        lax.all_to_all(
            row_peak.reshape(tp_count, local_rows, H), "tp", split_axis=0, concat_axis=0, tiled=True
        ),
        lax.all_to_all(
            weight_sum.reshape(tp_count, local_rows, H),
            "tp",
            split_axis=0,
            concat_axis=0,
            tiled=True,
        ),
    )
    overall = jnp.max(got_peaks, axis=0)
    factor = jnp.exp(got_peaks - overall[None])
    merged_sum = jnp.sum(got_sums * factor, axis=0)
    merged = jnp.sum(got_outputs * factor[:, :, :, None], axis=0) / merged_sum[:, :, None]
    attended = merged.reshape(local_rows, feature_width).astype(jnp.bfloat16)
    projected = jnp.dot(
        lax.all_gather(attended, "tp", axis=0, tiled=True),
        out_weight,
        preferred_element_type=jnp.float32,
    )
    level_hot = (jnp.arange(gate_table.shape[0], dtype=jnp.int32) == noise_level[0]).astype(
        jnp.float32
    )[None, :]
    gate_row = jnp.dot(level_hot, gate_table, precision=lax.Precision.HIGHEST)
    return (projected * gate_row).astype(jnp.bfloat16)[None]


MESH = pl.DeviceIdType.MESH


def fused_kernel(
    n,
    heads,
    mask_ref,
    blocks_ref,
    query_in,
    fresh_in,
    history_in,
    weight_in,
    gate_ref,
    out_ref,
    kv,
    queries,
    gathered,
    weight,
    bias,
    total,
    in_send,
    in_recv,
    pass_send,
    pass_recv,
    gather_send,
    gather_recv,
    local_sem,
):
    me = lax.axis_index("tp")
    core = lax.axis_index("stretch")
    partner = {"stretch": 1 - core}
    line = n // 2
    spot, side = me // 2, me % 2
    local_rows = query_in.shape[1]
    history_rows = history_in.shape[1]
    row_count = n * local_rows
    history_total = n * history_rows
    other_base = history_total
    own_base = history_total + row_count
    block_count = mask_ref.shape[1]

    barrier = pltpu.get_barrier_semaphore()
    for offset in range(1, n):
        pl.semaphore_signal(
            barrier, inc=1, device_id={"tp": lax.rem(me + offset, n)}, device_id_type=MESH
        )
    pl.semaphore_signal(barrier, inc=1, device_id=partner, device_id_type=MESH)
    pl.semaphore_wait(barrier, n)

    def remote(source, target, send, recv, device):
        return pltpu.make_async_remote_copy(
            src_ref=source,
            dst_ref=target,
            send_sem=send,
            recv_sem=recv,
            device_id=device,
            device_id_type=MESH,
        )

    def columns(owner, head):
        return pl.ds(pl.multiple_of((owner * heads + head) * HD, HD), HD)

    def history_span(source):
        return pl.ds(pl.multiple_of(source * history_rows, history_rows), history_rows)

    def fresh_span(base, source):
        return pl.ds(pl.multiple_of(base + source * local_rows, local_rows), local_rows)

    def inbound(head, source, target):
        wide = columns(target, head)
        device = {"tp": target}
        return (
            remote(
                history_in.at[core, :, wide],
                kv.at[head, core, history_span(source), :],
                in_send.at[0, head, target],
                in_recv.at[0, head, source],
                device,
            ),
            remote(
                fresh_in.at[:, 0, :, wide],
                kv.at[head, :, fresh_span(own_base, source), :],
                in_send.at[1, head, target],
                in_recv.at[1, head, source],
                device,
            ),
            remote(
                query_in.at[0, :, wide],
                queries.at[head, fresh_span(0, source), :],
                in_send.at[2, head, target],
                in_recv.at[2, head, source],
                device,
            ),
        )

    def passed_history(head, source, which):
        place = kv.at[head, which, history_span(source), :]
        return remote(
            place, place, pass_send.at[0, head, source], pass_recv.at[0, head, source], partner
        )

    def passed_fresh(head, source):
        return remote(
            kv.at[head, :, fresh_span(own_base, source), :],
            kv.at[head, :, fresh_span(other_base, source), :],
            pass_send.at[1, head, source],
            pass_recv.at[1, head, source],
            partner,
        )

    def own_fresh(head):
        return remote(
            fresh_in.at[:, 0, :, columns(me, head)],
            kv.at[head, :, fresh_span(other_base, me), :],
            pass_send.at[1, head, me],
            pass_recv.at[1, head, me],
            partner,
        )

    def local_copies(head):
        wide = columns(me, head)
        pairs = (
            (history_in.at[:, :, wide], kv.at[head, :, history_span(me), :]),
            (fresh_in.at[:, 0, :, wide], kv.at[head, :, fresh_span(own_base, me), :]),
            (query_in.at[0, :, wide], queries.at[head, fresh_span(0, me), :]),
            (weight_in.at[:, head], weight.at[head]),
        )
        return [
            pltpu.make_async_copy(source, target, local_sem.at[place, head])
            for place, (source, target) in enumerate(pairs)
        ]

    for head in range(heads):
        for offset in range(1, n):
            for copy in inbound(head, me, lax.rem(me + offset, n)):
                copy.start()
        own_fresh(head).start()
        for copy in local_copies(head):
            copy.start()

    live = blocks_ref[0] * BLK
    positions = lax.broadcasted_iota(jnp.int32, (1, history_total), 1)
    history_bias = jnp.where(positions < live, 0.0, NEGATIVE)
    for block in range(block_count):
        bias[block : block + 1, 0:history_total] = history_bias
        for column in range(2 * block_count):
            shown = jnp.full((1, BLK), mask_ref[0, block, column], jnp.int32)
            begin = history_total + column * BLK
            bias[block : block + 1, begin : begin + BLK] = jnp.where(shown > 0, 0.0, NEGATIVE)

    unit = math.log2(math.e) / math.sqrt(HD)

    def attend(head):
        def step(block, carry):
            rows = pl.ds(pl.multiple_of(block * BLK, BLK), BLK)
            scores = lax.dot_general(
                queries[head, rows, :],
                kv[head, 0],
                (((1,), (1,)), ((), ())),
                preferred_element_type=jnp.float32,
            )
            scores = scores * unit + bias[pl.ds(block, 1), :]
            peak = jnp.max(scores, axis=1, keepdims=True)
            weights = jnp.exp2(scores - peak)
            weight_sum = jnp.sum(weights, axis=1, keepdims=True)
            output = jnp.dot(
                weights.astype(jnp.bfloat16), kv[head, 1], preferred_element_type=jnp.float32
            )
            gathered[head, me, rows, :] = (output / weight_sum).astype(jnp.bfloat16)
            return carry

        lax.fori_loop(0, block_count, step, 0)

    def hop(head, block, way):
        place = gathered.at[head, block]
        target = (me + 2, me - 2, me + 1 - 2 * side)[way]
        return remote(
            place,
            place,
            gather_send.at[way, head, block],
            gather_recv.at[head, block],
            {"tp": target},
        )

    def launch(head, block, up, down):
        if up:
            pl.when(spot < line - 1)(lambda: hop(head, block, 0).start())
        if down:
            pl.when(spot > 0)(lambda: hop(head, block, 1).start())
        hop(head, block, 2).start()

    def relay(head):
        for far in range(1, line):

            @pl.when(spot >= far)
            def _():
                block = me - 2 * far
                hop(head, block, 2).wait_recv()
                launch(head, block, True, False)

            @pl.when(spot + far < line)
            def _():
                block = me + 2 * far
                hop(head, block, 2).wait_recv()
                launch(head, block, False, True)

    def finish(head):
        for place in range(line):
            hop(head, 2 * place + 1 - side, 2).wait_recv()

    def project(head):
        last = head == heads - 1

        def step(block, carry):
            rows = pl.ds(pl.multiple_of(block * BLK, BLK), BLK)
            left = jnp.concatenate([gathered[head, source, rows, :] for source in range(n)], axis=1)
            right = weight[head].reshape(n * HD, weight.shape[3])
            part = jnp.dot(left, right, preferred_element_type=jnp.float32)
            if head > 0:
                part = part + total[rows, :]
            if last:
                out_ref[0, rows, :] = (part * gate_ref[...]).astype(out_ref.dtype)
            else:
                total[rows, :] = part
            return carry

        lax.fori_loop(0, block_count, step, 0)

    for head in range(heads):
        mine = local_copies(head)
        for copy in mine[:3]:
            copy.wait()
        for offset in range(1, n):
            source = lax.rem(me + n - offset, n)
            arrivals = inbound(head, source, me)
            arrivals[0].wait_recv()
            passed_history(head, source, core).start()
            arrivals[1].wait_recv()
            passed_fresh(head, source).start()
            arrivals[2].wait_recv()
        for offset in range(1, n):
            source = lax.rem(me + n - offset, n)
            passed_history(head, source, 1 - core).wait_recv()
            passed_fresh(head, source).wait_recv()
        own_fresh(head).wait_recv()
        attend(head)
        launch(head, me, True, True)
        if head > 0:
            relay(head - 1)
            finish(head - 1)
            local_copies(head - 1)[3].wait()
            project(head - 1)
    relay(heads - 1)
    finish(heads - 1)
    local_copies(heads - 1)[3].wait()
    project(heads - 1)

    for head in range(heads):
        for offset in range(1, n):
            source = lax.rem(me + n - offset, n)
            for copy in inbound(head, me, lax.rem(me + offset, n)):
                copy.wait_send()
            passed_history(head, source, core).wait_send()
            passed_fresh(head, source).wait_send()
        own_fresh(head).wait_send()
        for way, allowed in ((0, spot < line - 1), (1, spot > 0)):

            @pl.when(allowed)
            def _():
                hop(head, me, way).wait_send()

        hop(head, me, 2).wait_send()
        for far in range(1, line):

            @pl.when(spot >= far)
            def _():
                block = me - 2 * far
                pl.when(spot < line - 1)(lambda: hop(head, block, 0).wait_send())
                hop(head, block, 2).wait_send()

            @pl.when(spot + far < line)
            def _():
                block = me + 2 * far
                pl.when(spot > 0)(lambda: hop(head, block, 1).wait_send())
                hop(head, block, 2).wait_send()


def on_device_fused(
    query, stretch_kv, history_kv, block_mask, noise_level, history_blocks, out_weight, gate_table
):
    n = lax.axis_size("tp")
    heads = H // n
    local_rows, history_rows = query.shape[1], history_kv.shape[1]
    row_count = n * local_rows
    key_count = n * history_rows + 2 * row_count
    wide = out_weight.shape[1]
    block_count = block_mask.shape[1]
    gate_row = lax.dynamic_slice(gate_table, (noise_level[0], 0), (1, wide))
    anywhere = pl.BlockSpec(memory_space=pl.ANY)
    scalars = pl.BlockSpec(memory_space=pltpu.SMEM)
    vector = pl.BlockSpec(memory_space=pltpu.VMEM)
    dma = pltpu.SemaphoreType.DMA
    return pl.pallas_call(
        functools.partial(fused_kernel, n, heads),
        out_shape=jax.ShapeDtypeStruct((1, row_count, wide), jnp.bfloat16),
        in_specs=[scalars, scalars, anywhere, anywhere, anywhere, anywhere, vector],
        out_specs=vector,
        scratch_shapes=[
            pltpu.VMEM((heads, 2, key_count, HD), jnp.bfloat16),
            pltpu.VMEM((heads, row_count, HD), jnp.bfloat16),
            pltpu.VMEM((heads, n, row_count, HD), jnp.bfloat16),
            pltpu.VMEM((heads, n, HD, wide), jnp.bfloat16),
            pltpu.VMEM((block_count, key_count), jnp.float32),
            pltpu.VMEM((row_count, wide), jnp.float32),
            dma((3, heads, n)),
            dma((3, heads, n)),
            dma((2, heads, n)),
            dma((2, heads, n)),
            dma((3, heads, n)),
            dma((heads, n)),
            dma((4, heads)),
        ],
        compiler_params=pltpu.CompilerParams(
            collective_id=0, has_side_effects=True, vmem_limit_bytes=60 * 1024 * 1024
        ),
    )(
        block_mask,
        history_blocks,
        query,
        stretch_kv,
        history_kv,
        out_weight.reshape(n, heads, HD, wide),
        gate_row,
    )


def solution(mesh):
    count = mesh.shape["tp"]
    fits = H % count == 0 and count % 2 == 0 and mesh.shape["stretch"] == 2
    return jax.shard_map(
        on_device_fused if fits else on_device,
        mesh=mesh,
        in_specs=(
            P(("rep", "stretch"), "tp", None),
            P(None, ("rep", "stretch"), "tp", None),
            P(None, ("rep", "tp"), None),
            P(("rep", "stretch"), None, None),
            P(("rep", "stretch")),
            P("rep"),
            P(None, "tp"),
            P(None, "tp"),
        ),
        out_specs=P(("rep", "stretch"), None, "tp"),
        check_vma=False,
    )
```

```python
import functools
import math

import jax
import jax.numpy as jnp
from jax import lax
from jax.experimental import pallas as pl
from jax.experimental.pallas import tpu as pltpu
from jax.sharding import PartitionSpec as P

H = 24
HD = 128
BLK = 128


NEGATIVE = -1e30


def shifted(value, axis, steps):
    count = lax.axis_size(axis)
    first, last = (max(0, -steps), min(count, count - steps))
    return lax.ppermute(value, axis, [(source, source + steps) for source in range(first, last)])


def head_block(queries, key_rows, value_rows, allowed):
    key_count = key_rows.shape[0]
    head_count = queries.shape[1]
    key_heads = key_rows.reshape(key_count, head_count, HD)
    scores = jnp.einsum("qhd,khd->qhk", queries, key_heads, preferred_element_type=jnp.float32) * (
        1.0 / math.sqrt(HD)
    )
    scores = jnp.where(allowed[:, None, :], scores, NEGATIVE)
    row_peak = jnp.max(scores, axis=2)
    weights = jnp.where(allowed[:, None, :], jnp.exp(scores - row_peak[:, :, None]), 0.0)
    weight_sum = jnp.sum(weights, axis=2)
    output = None
    value_heads = value_rows.reshape(key_count, head_count, HD).astype(jnp.float32)
    output = jnp.einsum("qhk,khd->qhd", weights, value_heads, precision=lax.Precision.HIGHEST)
    return (row_peak, weight_sum, output)


def combine(earlier, later):
    row_peak = jnp.maximum(earlier[0], later[0])
    scale_one = jnp.exp(earlier[0] - row_peak)
    scale_two = jnp.exp(later[0] - row_peak)
    weight_sum = earlier[1] * scale_one + later[1] * scale_two
    output = None
    output = earlier[2] * scale_one[:, :, None] + later[2] * scale_two[:, :, None]
    return (row_peak, weight_sum, output)


def column_table(columns, block_count):
    return (columns[:, None] == jnp.arange(2 * block_count, dtype=jnp.int32)[None, :]).astype(
        jnp.float32
    )


def attend_all(
    queries,
    query_positions,
    fresh_keys,
    fresh_values,
    fresh_hot,
    mask_table,
    history_pair,
    history_live,
    span,
):
    row_count = queries.shape[0]
    head_count = queries.shape[1]
    block_count = mask_table.shape[0]
    query_hot = (
        (query_positions // BLK)[:, None] == jnp.arange(block_count, dtype=jnp.int32)[None, :]
    ).astype(jnp.float32)
    fresh_allowed = jnp.dot(jnp.dot(query_hot, mask_table), fresh_hot.T) > 0.5
    base_peak = jnp.full((row_count, head_count), NEGATIVE, jnp.float32)
    skipped = (
        base_peak,
        jnp.zeros((row_count, head_count), jnp.float32),
        jnp.zeros((row_count, head_count, HD), jnp.float32),
    )
    result = head_block(queries, fresh_keys, fresh_values, fresh_allowed)
    for sub_block in range(history_pair.shape[1] // span):
        lower_row = sub_block * span
        key_rows = history_pair[0, lower_row : lower_row + span]
        value_rows = history_pair[1, lower_row : lower_row + span]
        live_rows = history_live[lower_row : lower_row + span]
        allowed = jnp.broadcast_to(live_rows[None, :], (row_count, span))
        block_part = lax.cond(
            jnp.any(live_rows),
            lambda: head_block(queries, key_rows, value_rows, allowed),
            lambda: skipped,
        )
        result = combine(result, block_part)
    return result


def on_device(
    query, stretch_kv, history_kv, block_mask, noise_level, history_blocks, out_weight, gate_table
):
    tp_count = lax.axis_size("tp")
    tp_index = lax.axis_index("tp")
    local_rows = query.shape[1]
    feature_width = query.shape[2]
    history_rows = history_kv.shape[1]
    block_count = block_mask.shape[1]
    own_pair = stretch_kv[:, 0]
    older_pair = shifted(own_pair, "stretch", 1)
    mask_table = block_mask[0].astype(jnp.float32)
    live_limit = history_blocks[0] * BLK
    fresh_keys = jnp.concatenate([older_pair[0], own_pair[0]], 0)
    fresh_values = jnp.concatenate([older_pair[1], own_pair[1]], 0)
    own_positions = tp_index * local_rows + jnp.arange(local_rows, dtype=jnp.int32)
    fresh_hot = column_table(
        jnp.concatenate([own_positions // BLK, block_count + own_positions // BLK], 0), block_count
    )
    history_positions = tp_index * history_rows + jnp.arange(history_rows, dtype=jnp.int32)
    history_live = history_positions < live_limit
    piece = lax.all_gather(query[0], "tp", axis=0, tiled=True)
    row_count = piece.shape[0]
    positions = jnp.arange(row_count, dtype=jnp.int32)
    row_peak, weight_sum, output = attend_all(
        piece.reshape(row_count, H, HD),
        positions,
        fresh_keys,
        fresh_values,
        fresh_hot,
        mask_table,
        history_kv,
        history_live,
        BLK,
    )
    got_outputs, got_peaks, got_sums = (
        lax.all_to_all(
            output.reshape(tp_count, local_rows, H, HD),
            "tp",
            split_axis=0,
            concat_axis=0,
            tiled=True,
        ),
        lax.all_to_all(
            row_peak.reshape(tp_count, local_rows, H), "tp", split_axis=0, concat_axis=0, tiled=True
        ),
        lax.all_to_all(
            weight_sum.reshape(tp_count, local_rows, H),
            "tp",
            split_axis=0,
            concat_axis=0,
            tiled=True,
        ),
    )
    overall = jnp.max(got_peaks, axis=0)
    factor = jnp.exp(got_peaks - overall[None])
    merged_sum = jnp.sum(got_sums * factor, axis=0)
    merged = jnp.sum(got_outputs * factor[:, :, :, None], axis=0) / merged_sum[:, :, None]
    attended = merged.reshape(local_rows, feature_width).astype(jnp.bfloat16)
    projected = jnp.dot(
        lax.all_gather(attended, "tp", axis=0, tiled=True),
        out_weight,
        preferred_element_type=jnp.float32,
    )
    level_hot = (jnp.arange(gate_table.shape[0], dtype=jnp.int32) == noise_level[0]).astype(
        jnp.float32
    )[None, :]
    gate_row = jnp.dot(level_hot, gate_table, precision=lax.Precision.HIGHEST)
    return (projected * gate_row).astype(jnp.bfloat16)[None]


MESH = pl.DeviceIdType.MESH
WINDOW = 3
PIECES = 2
LAG = 0


def exchange_order(n):
    far, near = list(range(n // 2, n)), list(range(1, n // 2))
    order = []
    for place, code in enumerate(far):
        order += [code] + near[place : place + 1]
    return order


def crossed(me, code, n):
    partner, bit = 0, 1
    while bit < n:
        digit = lax.rem(me // bit, 2)
        partner = partner + bit * (1 - digit if code & bit else digit)
        bit *= 2
    return partner


def fused_kernel(
    n,
    heads,
    mask_ref,
    blocks_ref,
    query_in,
    fresh_in,
    history_in,
    weight_in,
    gate_ref,
    out_ref,
    kv,
    queries,
    gathered,
    weight,
    bias,
    total,
    in_send,
    in_recv,
    pass_send,
    pass_recv,
    gather_send,
    gather_recv,
    local_sem,
):
    me = lax.axis_index("tp")
    core = lax.axis_index("stretch")
    partner = {"stretch": 1 - core}
    line = n // 2
    spot, side = me // 2, me % 2
    local_rows = query_in.shape[1]
    history_rows = history_in.shape[1]
    row_count = n * local_rows
    history_total = n * history_rows
    other_base = history_total
    own_base = history_total + row_count
    block_count = mask_ref.shape[1]
    piece_blocks = block_count // PIECES
    piece_rows = piece_blocks * BLK

    barrier = pltpu.get_barrier_semaphore()
    for offset in range(1, n):
        pl.semaphore_signal(
            barrier, inc=1, device_id={"tp": lax.rem(me + offset, n)}, device_id_type=MESH
        )
    pl.semaphore_signal(barrier, inc=1, device_id=partner, device_id_type=MESH)
    pl.semaphore_wait(barrier, n)

    def remote(source, target, send, recv, device):
        return pltpu.make_async_remote_copy(
            src_ref=source,
            dst_ref=target,
            send_sem=send,
            recv_sem=recv,
            device_id=device,
            device_id_type=MESH,
        )

    def columns(owner, head):
        return pl.ds(pl.multiple_of((owner * heads + head) * HD, HD), HD)

    def history_span(source):
        return pl.ds(pl.multiple_of(source * history_rows, history_rows), history_rows)

    def fresh_span(base, source):
        return pl.ds(pl.multiple_of(base + source * local_rows, local_rows), local_rows)

    def inbound(head, source, target):
        wide = columns(target, head)
        device = {"tp": target}
        return (
            remote(
                history_in.at[core, :, wide],
                kv.at[head, core, history_span(source), :],
                in_send.at[0, head, target],
                in_recv.at[0, head, source],
                device,
            ),
            remote(
                fresh_in.at[:, 0, :, wide],
                kv.at[head, :, fresh_span(own_base, source), :],
                in_send.at[1, head, target],
                in_recv.at[1, head, source],
                device,
            ),
            remote(
                query_in.at[0, :, wide],
                queries.at[head, fresh_span(0, source), :],
                in_send.at[2, head, target],
                in_recv.at[2, head, source],
                device,
            ),
        )

    def passed_history(head, source, which):
        place = kv.at[head, which, history_span(source), :]
        return remote(
            place, place, pass_send.at[0, head, source], pass_recv.at[0, head, source], partner
        )

    def passed_fresh(head, source):
        return remote(
            kv.at[head, :, fresh_span(own_base, source), :],
            kv.at[head, :, fresh_span(other_base, source), :],
            pass_send.at[1, head, source],
            pass_recv.at[1, head, source],
            partner,
        )

    def own_fresh(head):
        return remote(
            fresh_in.at[:, 0, :, columns(me, head)],
            kv.at[head, :, fresh_span(other_base, me), :],
            pass_send.at[1, head, me],
            pass_recv.at[1, head, me],
            partner,
        )

    def local_copy(head, place):
        wide = columns(me, head)
        source, target = (
            (history_in.at[:, :, wide], kv.at[head, :, history_span(me), :]),
            (fresh_in.at[:, 0, :, wide], kv.at[head, :, fresh_span(own_base, me), :]),
            (query_in.at[0, :, wide], queries.at[head, fresh_span(0, me), :]),
            (weight_in.at[:, head], weight.at[head]),
        )[place]
        return pltpu.make_async_copy(source, target, local_sem.at[place, head])

    peers = [crossed(me, code, n) for code in exchange_order(n)]
    steps = [(head, peer) for head in range(heads) for peer in peers]

    def send_step(index):
        if index < len(steps):
            head, peer = steps[index]
            for copy in inbound(head, me, peer):
                copy.start()

    for index in range(WINDOW):
        send_step(index)
    for head in range(heads):
        own_fresh(head).start()
        for place in range(4):
            local_copy(head, place).start()

    live = blocks_ref[0] * BLK
    positions = lax.broadcasted_iota(jnp.int32, (1, history_total), 1)
    history_bias = jnp.where(positions < live, 0.0, NEGATIVE)
    for block in range(block_count):
        bias[block : block + 1, 0:history_total] = history_bias
        for column in range(2 * block_count):
            shown = jnp.full((1, BLK), mask_ref[0, block, column], jnp.int32)
            begin = history_total + column * BLK
            bias[block : block + 1, begin : begin + BLK] = jnp.where(shown > 0, 0.0, NEGATIVE)

    unit = math.log2(math.e) / math.sqrt(HD)

    def attend(head, piece):
        def step(block, carry):
            rows = pl.ds(pl.multiple_of(block * BLK, BLK), BLK)
            scores = lax.dot_general(
                queries[head, rows, :],
                kv[head, 0],
                (((1,), (1,)), ((), ())),
                preferred_element_type=jnp.float32,
            )
            scores = scores * unit + bias[pl.ds(block, 1), :]
            peak = jnp.max(scores, axis=1, keepdims=True)
            weights = jnp.exp2(scores - peak)
            weight_sum = jnp.sum(weights, axis=1, keepdims=True)
            output = jnp.dot(
                weights.astype(jnp.bfloat16), kv[head, 1], preferred_element_type=jnp.float32
            )
            gathered[head, me, rows, :] = (output / weight_sum).astype(jnp.bfloat16)
            return carry

        lax.fori_loop(piece * piece_blocks, (piece + 1) * piece_blocks, step, 0)

    def hop(head, block, way, piece):
        place = gathered.at[head, block, piece * piece_rows : (piece + 1) * piece_rows, :]
        target = (me + 2, me - 2, me + 1 - 2 * side)[way]
        return remote(
            place,
            place,
            gather_send.at[way, head, block * PIECES + piece],
            gather_recv.at[head, block * PIECES + piece],
            {"tp": target},
        )

    def launch(head, block, up, down, piece):
        if up:
            pl.when(spot < line - 1)(lambda: hop(head, block, 0, piece).start())
        if down:
            pl.when(spot > 0)(lambda: hop(head, block, 1, piece).start())
        hop(head, block, 2, piece).start()

    def relay(head, far, piece):
        @pl.when(spot >= far)
        def _():
            block = me - 2 * far
            hop(head, block, 2, piece).wait_recv()
            launch(head, block, True, False, piece)

        @pl.when(spot + far < line)
        def _():
            block = me + 2 * far
            hop(head, block, 2, piece).wait_recv()
            launch(head, block, False, True, piece)

    def finish(head, piece):
        for place in range(line):
            hop(head, 2 * place + 1 - side, 2, piece).wait_recv()

    def project(head, piece):
        last = head == heads - 1

        def step(block, carry):
            rows = pl.ds(pl.multiple_of(block * BLK, BLK), BLK)
            left = jnp.concatenate([gathered[head, source, rows, :] for source in range(n)], axis=1)
            right = weight[head].reshape(n * HD, weight.shape[3])
            part = jnp.dot(left, right, preferred_element_type=jnp.float32)
            if head > 0:
                part = part + total[rows, :]
            if last:
                out_ref[0, rows, :] = (part * gate_ref[...]).astype(out_ref.dtype)
            else:
                total[rows, :] = part
            return carry

        lax.fori_loop(piece * piece_blocks, (piece + 1) * piece_blocks, step, 0)

    relay_after = {len(peers) - 1 - 2 * (line - 1 - LAG - far): far for far in range(1, line - LAG)}
    for head in range(heads):
        for place in range(3):
            local_copy(head, place).wait()
        for place, source in enumerate(peers):
            arrivals = inbound(head, source, me)
            arrivals[0].wait_recv()
            passed_history(head, source, core).start()
            arrivals[1].wait_recv()
            passed_fresh(head, source).start()
            arrivals[2].wait_recv()
            send_step(head * len(peers) + place + WINDOW)
            if head > 0 and place in relay_after:
                for piece in range(PIECES):
                    relay(head - 1, relay_after[place], piece)
        for source in peers:
            passed_history(head, source, 1 - core).wait_recv()
            passed_fresh(head, source).wait_recv()
        own_fresh(head).wait_recv()
        for piece in range(PIECES):
            attend(head, piece)
            launch(head, me, True, True, piece)
        if head > 0:
            if LAG:
                for piece in range(PIECES):
                    relay(head - 1, line - 1, piece)
            local_copy(head - 1, 3).wait()
            for piece in range(PIECES):
                finish(head - 1, piece)
                project(head - 1, piece)
    for far in range(1, line):
        for piece in range(PIECES):
            relay(heads - 1, far, piece)
    local_copy(heads - 1, 3).wait()
    for piece in range(PIECES):
        finish(heads - 1, piece)
        project(heads - 1, piece)

    for head in range(heads):
        for source in peers:
            for copy in inbound(head, me, source):
                copy.wait_send()
            passed_history(head, source, core).wait_send()
            passed_fresh(head, source).wait_send()
        own_fresh(head).wait_send()
        for piece in range(PIECES):

            @pl.when(spot < line - 1)
            def _():
                hop(head, me, 0, piece).wait_send()

            @pl.when(spot > 0)
            def _():
                hop(head, me, 1, piece).wait_send()

            hop(head, me, 2, piece).wait_send()
            for far in range(1, line):

                @pl.when(spot >= far)
                def _():
                    block = me - 2 * far
                    pl.when(spot < line - 1)(lambda: hop(head, block, 0, piece).wait_send())
                    hop(head, block, 2, piece).wait_send()

                @pl.when(spot + far < line)
                def _():
                    block = me + 2 * far
                    pl.when(spot > 0)(lambda: hop(head, block, 1, piece).wait_send())
                    hop(head, block, 2, piece).wait_send()


def on_device_fused(
    query, stretch_kv, history_kv, block_mask, noise_level, history_blocks, out_weight, gate_table
):
    n = lax.axis_size("tp")
    heads = H // n
    local_rows, history_rows = query.shape[1], history_kv.shape[1]
    row_count = n * local_rows
    key_count = n * history_rows + 2 * row_count
    wide = out_weight.shape[1]
    block_count = block_mask.shape[1]
    gate_row = lax.dynamic_slice(gate_table, (noise_level[0], 0), (1, wide))
    anywhere = pl.BlockSpec(memory_space=pl.ANY)
    scalars = pl.BlockSpec(memory_space=pltpu.SMEM)
    vector = pl.BlockSpec(memory_space=pltpu.VMEM)
    dma = pltpu.SemaphoreType.DMA
    return pl.pallas_call(
        functools.partial(fused_kernel, n, heads),
        out_shape=jax.ShapeDtypeStruct((1, row_count, wide), jnp.bfloat16),
        in_specs=[scalars, scalars, anywhere, anywhere, anywhere, anywhere, vector],
        out_specs=vector,
        scratch_shapes=[
            pltpu.VMEM((heads, 2, key_count, HD), jnp.bfloat16),
            pltpu.VMEM((heads, row_count, HD), jnp.bfloat16),
            pltpu.VMEM((heads, n, row_count, HD), jnp.bfloat16),
            pltpu.VMEM((heads, n, HD, wide), jnp.bfloat16),
            pltpu.VMEM((block_count, key_count), jnp.float32),
            pltpu.VMEM((row_count, wide), jnp.float32),
            dma((3, heads, n)),
            dma((3, heads, n)),
            dma((2, heads, n)),
            dma((2, heads, n)),
            dma((3, heads, n * PIECES)),
            dma((heads, n * PIECES)),
            dma((4, heads)),
        ],
        compiler_params=pltpu.CompilerParams(
            collective_id=0, has_side_effects=True, vmem_limit_bytes=60 * 1024 * 1024
        ),
    )(
        block_mask,
        history_blocks,
        query,
        stretch_kv,
        history_kv,
        out_weight.reshape(n, heads, HD, wide),
        gate_row,
    )


def solution(mesh):
    count = mesh.shape["tp"]
    fits = H % count == 0 and count & (count - 1) == 0 and count > 2 and mesh.shape["stretch"] == 2
    return jax.shard_map(
        on_device_fused if fits else on_device,
        mesh=mesh,
        in_specs=(
            P(("rep", "stretch"), "tp", None),
            P(None, ("rep", "stretch"), "tp", None),
            P(None, ("rep", "tp"), None),
            P(("rep", "stretch"), None, None),
            P(("rep", "stretch")),
            P("rep"),
            P(None, "tp"),
            P(None, "tp"),
        ),
        out_specs=P(("rep", "stretch"), None, "tp"),
        check_vma=False,
    )
```
